32 devices in a mesh: group: 2 (over y), view: 4 (over z), depth: 2 (over x), row: 2 (over core).
Axes of the slice: x: 2, y: 2, z: 4, core: 2. Of those that a mesh axis runs over, the one named last changes fastest.
Arguments:
- features: float32 [4, 32, 8, 512], P('view', None, ('group', 'row')), parts along dimension 2, may hold values from -6 to 6
- cotangent: float32 [8, 32, 8, 512], P('depth', 'view', ('group', 'row')), parts along dimension 2, may hold values from -6 to 6
- src_row: int32 [4, 8, 8, 512], P('view', 'depth', ('group', 'row')), parts along dimension 2, may hold values from -2 to 4, as said below
- src_col: int32 [4, 8, 8, 512], P('view', 'depth', ('group', 'row')), parts along dimension 2, may hold values from 0 to 510
- fractions: int32 [2, 4, 8, 8, 512], P(None, 'view', 'depth', ('group', 'row')), parts along dimension 3, may hold values from 0 to 256
Outputs:
- grad_features: float32 [4, 32, 8, 512], P('view', None, ('group', 'row'), 'depth'), parts along dimension 2
The draws below stay inside these ranges and needn't reach their ends.
There are 2 independent parts, one for each index of `group`. The reference program is written for one: setup_inputs(seed, part) draws one part's arguments, and reference() takes and returns one part's arrays. A program takes and returns all parts, laid end to end along the dimension named above; each array names one. Nothing has to cross between parts.
Inputs may be any that keep to these rules, and one draw needn't show every extreme that they name: src_row[v, d, y, x] lies between y - 2 and y + 1.
All inputs are finite; a program needn't handle non-finite values.
Results may differ from the reference program's by a relative error of at most 0.0003.
Values sent between devices are 32-bit elements; how exact they have to be, the bound alone decides.
A program may use at most 64 MiB of HBM per device.

```python
import jax
import jax.numpy as jnp
from jax import lax

C = 32
WC = 512
HALO = 2
VIEWS = 4
DEPTHS = 8
H = 4


def draw_src_row(key, part):
    shape_all = (VIEWS, DEPTHS, H, WC)
    offsets = jax.random.randint(jax.random.fold_in(key, 7), shape_all, -HALO, HALO)
    offsets = offsets.at[:, :, :, 0].set(-HALO).at[:, :, :, 1].set(HALO - 1)
    pixel_rows = lax.broadcasted_iota(jnp.int32, shape_all, 2)
    return (pixel_rows + offsets).astype(jnp.int32)


def draw_src_col(key, part):
    shape_all = (VIEWS, DEPTHS, H, WC)
    key_one, key_two = jax.random.split(jax.random.fold_in(key, 11))
    shifts = jax.random.randint(key_one, (VIEWS, 1, 1, 1), 0, 5)
    jitter = jax.random.randint(key_two, shape_all, -2, 3)
    planes = lax.broadcasted_iota(jnp.int32, shape_all, 1)
    columns = lax.broadcasted_iota(jnp.int32, shape_all, 3)
    values = jnp.clip(columns - (planes + 1) * shifts + jitter, 0, WC - 2)
    values = values.at[:, :, 0, 0].set(0).at[:, :, 0, WC - 1].set(WC - 2)
    return values.astype(jnp.int32)


def with_ends(entries, rng, least, high):
    longest = entries.shape.index(max(entries.shape))
    spots = []
    for shift in (0, 1):
        where = [jax.random.randint(jax.random.fold_in(rng, axis), (), 0, length) for axis, length in enumerate(entries.shape)]
        where[longest] = (where[longest] + shift) % entries.shape[longest]
        spots.append(tuple(where))
    return entries.at[spots[0]].set(least).at[spots[1]].set(high)


def block_levels(own_key, extent, shards, low, top_value):
    factor_of, own = 1.0, jax.random.fold_in(own_key, 6)
    for axis_at, shards_of in shards:
        heights = jnp.exp(jax.random.uniform(jax.random.fold_in(own, axis_at), (shards_of,), jnp.float32, low / len(shards), top_value / len(shards)))
        factor_of = factor_of * jnp.repeat(heights, extent[axis_at] // shards_of).reshape([-1 if axis == axis_at else 1 for axis in range(len(extent))])
    return factor_of


def scatter_about(key, shape, scale, limit, pieces=(), kind=jnp.bfloat16):
    entries = scale * jax.random.normal(key, shape, jnp.float32)
    if pieces:
        entries = entries * block_levels(key, shape, pieces, -0.22, 0.18)
    return jnp.clip(entries, -limit, limit).astype(kind)


def setup_inputs(seed: int = 0, part: int = 0) -> dict:
    key_list = jax.random.split(jax.random.key(seed), 6)
    part_keys = jax.random.split(jax.random.fold_in(key_list[5], part), 6)
    return {
        "features": scatter_about(part_keys[0], (VIEWS, C, H, WC), 1.0, 6.0, ((0, 4), (2, 2)), jnp.float32),
        "cotangent": scatter_about(part_keys[1], (DEPTHS, C, H, WC), (VIEWS / 8), 6.0, ((0, 2), (1, 4), (2, 2)), jnp.float32),
        "src_row": draw_src_row(jax.random.fold_in(jax.random.fold_in(key_list[5], part), 71), part),
        "src_col": draw_src_col(jax.random.fold_in(jax.random.fold_in(key_list[5], part), 71), part),
        "fractions": with_ends(jax.random.randint(part_keys[4], (2, VIEWS, DEPTHS, H, WC), 0, 257), jax.random.fold_in(part_keys[4], 1), 0, 256).astype(jnp.int32),
    }


def sample(flattened, flat_index, frac_row, frac_col, width):
    def corner(shift_by):
        return jnp.take(flattened, flat_index + shift_by, axis=1)
    upper_mix = (1.0 - frac_col) * corner(0) + frac_col * corner(1)
    lower_mix = (1.0 - frac_col) * corner(width) + frac_col * corner(width + 1)
    mixed = (1.0 - frac_row) * upper_mix + frac_row * lower_mix
    return jnp.transpose(mixed, (1, 0, 2, 3))


def spread(grad_warp, flat_index, frac_row, frac_col, width, length):
    moved = jnp.transpose(grad_warp, (1, 0, 2, 3))
    channels = moved.shape[0]
    upper_part = (1.0 - frac_row) * moved
    lower_part = frac_row * moved
    result = jnp.zeros((channels, length), jnp.float32)
    result = result.at[:, flat_index].add((1.0 - frac_col) * upper_part)
    result = result.at[:, flat_index + 1].add(frac_col * upper_part)
    result = result.at[:, flat_index + width].add((1.0 - frac_col) * lower_part)
    result = result.at[:, flat_index + width + 1].add(frac_col * lower_part)
    return result


def reference(features, cotangent, src_row, src_col, fractions):
    padded = jnp.pad(features, ((0, 0), (0, 0), (HALO, HALO), (0, 0)))
    length = (H + 2 * HALO) * WC
    flattened_all = padded.reshape(VIEWS, C, length)
    weights = fractions.astype(jnp.float32) / 256.0

    def warp_view(index_view):
        flat_index = ((src_row[index_view] + HALO) * WC + src_col[index_view]).astype(jnp.int32)
        warped = sample(flattened_all[index_view], flat_index, weights[0, index_view], weights[1, index_view], WC)
        return warped, flat_index

    def accumulate(index_view, running):
        return running + warp_view(index_view)[0]

    view_sum = lax.fori_loop(0, VIEWS, accumulate, jnp.zeros((DEPTHS, C, H, WC), jnp.float32))
    average = view_sum / VIEWS
    factor = 2.0 / VIEWS

    def backward_view(index_view):
        warped, flat_index = warp_view(index_view)
        grad_warp = factor * cotangent * (warped - average)
        spread_out = spread(grad_warp, flat_index, weights[0, index_view], weights[1, index_view], WC, length)
        return spread_out.reshape(C, H + 2 * HALO, WC)[:, HALO:HALO + H]

    return lax.map(backward_view, jnp.arange(VIEWS, dtype=jnp.int32))
```

```python
import functools

import jax
import jax.numpy as jnp
from jax import lax
from jax.experimental import pallas as pl
from jax.experimental.pallas import tpu as pltpu
from jax.sharding import PartitionSpec as P

MESH = pl.DeviceIdType.MESH
F32 = jnp.float32
BF16 = jnp.bfloat16
TILE = 256
CHUNK = 64
KEEP_BYTES = 24 << 20


def split(value):
    high = value.astype(BF16)
    low = (value - high.astype(F32)).astype(BF16)
    return jnp.concatenate([high, low], axis=0)


def kernel(
    sizes, feat, cot, srow, scol, frac, out,
    fbuf, rbuf, cbuf, wbuf, cotv, lane_q, stack, fstack, mats, warp, rweight, total, outbuf, inbuf,
    local_sem, f_send, f_recv, i_send, i_recv, o_send, o_recv, o_local,
):
    views, depths, rows, cc, planes, rl, width, keep = sizes
    me = lax.axis_index("view")
    mx = lax.axis_index("depth")
    mr = lax.axis_index("row")
    height = rows * rl
    wx = width // depths
    factor = 2.0 / views

    def view_at(step):
        return lax.rem(me + step, views)

    def others(step):
        for dx in range(depths):
            for dr in range(rows):
                yield dx, dr, lax.rem(mx + dx, depths), lax.rem(mr + dr, rows)

    barrier = pltpu.get_barrier_semaphore()
    for dx, dr, x, r in others(0):
        if dx or dr:
            pl.semaphore_signal(barrier, inc=1, device_id={"view": me, "depth": x, "row": r}, device_id_type=MESH)

    @pl.loop(1, views)
    def _(step):
        for dx, dr, x, r in others(step):
            pl.semaphore_signal(
                barrier, inc=1, device_id={"view": view_at(step), "depth": x, "row": r}, device_id_type=MESH
            )

    local = [
        pltpu.make_async_copy(feat.at[0, pl.ds(me * cc, cc)], fbuf.at[me, mr], local_sem.at[0]),
        pltpu.make_async_copy(srow.at[0], rbuf.at[me], local_sem.at[1]),
        pltpu.make_async_copy(scol.at[0], cbuf.at[me], local_sem.at[2]),
        pltpu.make_async_copy(frac.at[:, 0], wbuf.at[me], local_sem.at[3]),
        pltpu.make_async_copy(cot, cotv, local_sem.at[4]),
    ]
    for copy in local:
        copy.start()
    for j in range(TILE // CHUNK):
        part = lax.broadcasted_iota(jnp.int32, (CHUNK, width), 0) + j * CHUNK
        lane_q[pl.ds(j * CHUNK, CHUNK), :] = part.astype(F32).astype(BF16)

    pl.semaphore_wait(barrier, views * depths * rows - 1)

    def feat_copy(step, dr):
        to, r = lax.rem(me + views - step, views), lax.rem(mr + dr, rows)
        return pltpu.make_async_remote_copy(
            src_ref=feat.at[0, pl.ds(to * cc, cc)], dst_ref=fbuf.at[me, mr],
            send_sem=f_send.at[step, dr], recv_sem=f_recv.at[step, dr],
            device_id={"view": to, "row": r}, device_id_type=MESH,
        )

    def index_copies(step):
        to = lax.rem(me + views - step, views)
        pairs = [(srow.at[0], rbuf.at[me]), (scol.at[0], cbuf.at[me]), (frac.at[:, 0], wbuf.at[me])]
        return [
            pltpu.make_async_remote_copy(
                src_ref=source, dst_ref=target,
                send_sem=i_send.at[step, at], recv_sem=i_recv.at[step, at],
                device_id={"view": to}, device_id_type=MESH,
            )
            for at, (source, target) in enumerate(pairs)
        ]

    for dr in range(1, rows):
        feat_copy(0, dr).start()

    @pl.loop(1, views)
    def _(step):
        for dr in range(rows):
            feat_copy(step, dr).start()
        for copy in index_copies(step):
            copy.start()

    row_of = (lax.broadcasted_iota(jnp.int32, (height * cc, width), 0) // cc).astype(F32)

    def build(slot, v, d, i):
        col = cbuf[v, d, pl.ds(i, 1), :].astype(F32)
        fx = (wbuf[v, 1, d, pl.ds(i, 1), :].astype(F32) / 256.0).astype(BF16)
        fx = jnp.broadcast_to(fx, (CHUNK, width))
        for t in range(width // TILE):
            c = jnp.broadcast_to((col - float(t * TILE)).astype(BF16), (CHUNK, width))
            for j in range(TILE // CHUNK):
                apart = (lane_q[pl.ds(j * CHUNK, CHUNK), :] - c) - fx
                mats[slot, pl.ds(t * TILE + j * CHUNK, CHUNK), :] = jnp.maximum(
                    BF16(1.0) - jnp.abs(apart), BF16(0.0)
                )

    def slot_of(v, d, i):
        return (v * planes + d) * rl + i if keep else i

    def forward(v):
        for s in range(rows):
            for i in range(rl):
                stack[pl.ds((s * rl + i) * cc, cc), :] = fbuf[v, s, :, i, :]
        fstack[...] = split(stack[...])

        @pl.loop(0, planes)
        def _(d):
            for i in range(rl):
                slot = slot_of(v, d, i)
                build(slot, v, d, i)
                row = rbuf[v, d, pl.ds(i, 1), :].astype(F32)
                fy = wbuf[v, 0, d, pl.ds(i, 1), :].astype(F32) / 256.0
                weight = jnp.maximum(1.0 - jnp.abs(row_of - (row + fy)), 0.0)
                both = jnp.dot(fstack[...], mats[slot], preferred_element_type=F32)
                mixed = (both[: height * cc] + both[height * cc :]) * weight
                warped = mixed[:cc]
                for h in range(1, height):
                    warped = warped + mixed[h * cc : (h + 1) * cc]
                warp[v, d, i] = warped

    for copy in local[:4]:
        copy.wait()
    for dr in range(1, rows):
        feat_copy(0, dr).wait_recv()
    forward(me)

    @pl.loop(1, views)
    def _(step):
        for dr in range(rows):
            feat_copy(step, dr).wait_recv()
        for copy in index_copies(step):
            copy.wait_recv()
        forward(view_at(step))

    local[4].wait()

    def out_copy(v, step, dx, dr):
        x, r = lax.rem(mx + dx, depths), lax.rem(mr + dr, rows)
        return pltpu.make_async_remote_copy(
            src_ref=outbuf.at[v, x, r], dst_ref=inbuf.at[me, mx, mr],
            send_sem=o_send.at[step, dx, dr], recv_sem=o_recv.at[step, dx, dr],
            device_id={"view": v, "depth": x, "row": r}, device_id_type=MESH,
        )

    @pl.loop(0, planes)
    def _(d):
        for i in range(rl):
            mean = lax.fori_loop(1, views, lambda v, run: run + warp[v, d, i], warp[0, d, i]) / views
            grad = factor * cotv[d, :, i, :]

            def each(v, _):
                warp[v, d, i] = grad * (warp[v, d, i] - mean)
                return 0

            lax.fori_loop(0, views, each, 0)

    def backward(v):
        total[...] = jnp.zeros_like(total)

        @pl.loop(0, planes)
        def _(d):
            for i in range(rl):
                slot = slot_of(v, d, i)
                if not keep:
                    build(slot, v, d, i)
                row = rbuf[v, d, pl.ds(i, 1), :].astype(F32)
                fy = wbuf[v, 0, d, pl.ds(i, 1), :].astype(F32) / 256.0
                weight = jnp.maximum(1.0 - jnp.abs(row_of - (row + fy)), 0.0)
                moved = jnp.concatenate([warp[v, d, i]] * height, axis=0) * weight
                both = lax.dot_general(
                    split(moved), mats[slot], (((1,), (1,)), ((), ())), preferred_element_type=F32
                )
                total[...] += both[: height * cc] + both[height * cc :]

        for x in range(depths):
            for s in range(rows):
                for i in range(rl):
                    outbuf[v, x, s, i] = total[pl.ds((s * rl + i) * cc, cc), pl.ds(x * wx, wx)]

    @pl.loop(1, views)
    def _(step):
        v = view_at(step)
        backward(v)
        for dx in range(depths):
            for dr in range(rows):
                out_copy(v, step, dx, dr).start()

    backward(me)
    for dx in range(depths):
        for dr in range(rows):
            if dx or dr:
                out_copy(me, 0, dx, dr).start()
    for dx in range(depths):
        for dr in range(rows):
            if dx or dr:
                out_copy(me, 0, dx, dr).wait_recv()

    @pl.loop(1, views)
    def _(step):
        for dx in range(depths):
            for dr in range(rows):
                out_copy(view_at(step), step, dx, dr).wait_recv()

    for i in range(rl):
        for u in range(views):
            piece = None
            for x in range(depths):
                for s in range(rows):
                    own = jnp.logical_and(jnp.logical_and(me == u, mx == x), mr == s)
                    term = jnp.where(own, outbuf[u, x, s, i], inbuf[u, x, s, i])
                    piece = term if piece is None else piece + term
            out[i, pl.ds(u * cc, cc), :] = piece

    for dr in range(1, rows):
        feat_copy(0, dr).wait_send()
    for dx in range(depths):
        for dr in range(rows):
            if dx or dr:
                out_copy(me, 0, dx, dr).wait_send()

    @pl.loop(1, views)
    def _(step):
        for dr in range(rows):
            feat_copy(step, dr).wait_send()
        for copy in index_copies(step):
            copy.wait_send()
        for dx in range(depths):
            for dr in range(rows):
                out_copy(view_at(step), step, dx, dr).wait_send()


def per_device(features, cotangent, src_row, src_col, fractions):
    views, depths, rows = (lax.axis_size(axis) for axis in ("view", "depth", "row"))
    channels, rl, width = features.shape[1:]
    planes, cc = cotangent.shape[:2]
    height, wx = rows * rl, width // depths
    matrices = views * planes * rl
    keep = matrices * width * width * 2 <= KEEP_BYTES
    sizes = (views, depths, rows, cc, planes, rl, width, keep)
    grad = pl.pallas_call(
        functools.partial(kernel, sizes),
        out_shape=jax.ShapeDtypeStruct((rl, channels, wx), F32),
        in_specs=[pl.BlockSpec(memory_space=pl.ANY)] * 5,
        out_specs=pl.BlockSpec(memory_space=pltpu.VMEM),
        scratch_shapes=[
            pltpu.VMEM((views, rows, cc, rl, width), F32),
            pltpu.VMEM((views, planes, rl, width), jnp.int32),
            pltpu.VMEM((views, planes, rl, width), jnp.int32),
            pltpu.VMEM((views, 2, planes, rl, width), jnp.int32),
            pltpu.VMEM((planes, cc, rl, width), F32),
            pltpu.VMEM((TILE, width), BF16),
            pltpu.VMEM((height * cc, width), F32),
            pltpu.VMEM((2 * height * cc, width), BF16),
            pltpu.VMEM((matrices if keep else rl, width, width), BF16),
            pltpu.VMEM((views, planes, rl, cc, width), F32),
            pltpu.VMEM((8, width), F32),
            pltpu.VMEM((height * cc, width), F32),
            pltpu.VMEM((views, depths, rows, rl, cc, wx), F32),
            pltpu.VMEM((views, depths, rows, rl, cc, wx), F32),
            pltpu.SemaphoreType.DMA((5,)),
            pltpu.SemaphoreType.DMA((views, rows)),
            pltpu.SemaphoreType.DMA((views, rows)),
            pltpu.SemaphoreType.DMA((views, 3)),
            pltpu.SemaphoreType.DMA((views, 3)),
            pltpu.SemaphoreType.DMA((views, depths, rows)),
            pltpu.SemaphoreType.DMA((views, depths, rows)),
            pltpu.SemaphoreType.DMA((1,)),
        ],
        compiler_params=pltpu.CompilerParams(
            collective_id=0, has_side_effects=True, vmem_limit_bytes=56 << 20
        ),
    )(features, cotangent, src_row, src_col, fractions)
    return jnp.transpose(grad, (1, 0, 2))[None]


def solution(mesh):
    in_specs = (
        P("view", None, ("group", "row"), None),
        P("depth", "view", ("group", "row"), None),
        P("view", "depth", ("group", "row"), None),
        P("view", "depth", ("group", "row"), None),
        P(None, "view", "depth", ("group", "row"), None),
    )
    out_specs = P("view", None, ("group", "row"), "depth")
    return jax.shard_map(
        per_device, mesh=mesh, in_specs=in_specs, out_specs=out_specs, check_vma=False
    )
```

```python
import functools

import jax
import jax.numpy as jnp
from jax import lax
from jax.experimental import pallas as pl
from jax.experimental.pallas import tpu as pltpu
from jax.sharding import PartitionSpec as P

MESH = pl.DeviceIdType.MESH
F32 = jnp.float32
BF16 = jnp.bfloat16
TILE = 256
CHUNK = 64
KEEP_BYTES = 24 << 20


def split(value):
    high = value.astype(BF16)
    low = (value - high.astype(F32)).astype(BF16)
    return jnp.concatenate([high, low], axis=0)


def kernel(
    sizes, feat, cot, srow, scol, frac, out,
    fown, fbuf, rbuf, cbuf, wbuf, cotv, lane_q, stack, mats, warp, wsum, cotg, outbuf, pbuf, red, inbuf,
    local_sem, f_send, f_recv, p_send, p_recv, i_send, i_recv, d_send, d_recv, o_send, o_recv,
):
    views, depths, rows, cc, planes, rl, width, keep = sizes
    me = lax.axis_index("view")
    mx = lax.axis_index("depth")
    mr = lax.axis_index("row")
    height = rows * rl
    wx = width // depths
    factor = 2.0 / views

    def view_at(step):
        return lax.rem(me + step, views)

    def row_at(step):
        return lax.rem(mr + step, rows)

    def depth_at(step):
        return lax.rem(mx + step, depths)

    barrier = pltpu.get_barrier_semaphore()

    def greet(v, x, r):
        pl.semaphore_signal(
            barrier, inc=1, device_id={"view": v, "depth": x, "row": r}, device_id_type=MESH
        )

    @pl.loop(1, views)
    def _(step):
        for dx in range(depths):
            greet(view_at(step), depth_at(dx), mr)

    for dx in range(1, depths):
        greet(me, depth_at(dx), mr)
    for dr in range(1, rows):
        greet(me, mx, row_at(dr))

    local = [
        pltpu.make_async_copy(feat.at[0], fown, local_sem.at[0]),
        pltpu.make_async_copy(feat.at[0, pl.ds(me * cc, cc)], fbuf.at[me, mr], local_sem.at[1]),
        pltpu.make_async_copy(srow.at[0], rbuf.at[me], local_sem.at[2]),
        pltpu.make_async_copy(scol.at[0], cbuf.at[me], local_sem.at[3]),
        pltpu.make_async_copy(frac.at[:, 0], wbuf.at[me], local_sem.at[4]),
        pltpu.make_async_copy(cot, cotv, local_sem.at[5]),
    ]
    for copy in local:
        copy.start()
    for j in range(TILE // CHUNK):
        part = lax.broadcasted_iota(jnp.int32, (CHUNK, width), 0) + j * CHUNK
        lane_q[pl.ds(j * CHUNK, CHUNK), :] = part.astype(F32).astype(BF16)
    row_of = (lax.broadcasted_iota(jnp.int32, (height * cc, width), 0) // cc).astype(F32)

    def feat_copy(step):
        to = lax.rem(me + views - step, views)
        return pltpu.make_async_remote_copy(
            src_ref=fown.at[pl.ds(to * cc, cc)], dst_ref=fbuf.at[me, mr],
            send_sem=f_send.at[step], recv_sem=f_recv.at[step],
            device_id={"view": to}, device_id_type=MESH,
        )

    def pass_copy(step, dr):
        block = fbuf.at[view_at(step), mr]
        return pltpu.make_async_remote_copy(
            src_ref=block, dst_ref=block,
            send_sem=p_send.at[step, dr], recv_sem=p_recv.at[step, dr],
            device_id={"row": row_at(dr)}, device_id_type=MESH,
        )

    def index_copies(step):
        to = lax.rem(me + views - step, views)
        return [
            pltpu.make_async_remote_copy(
                src_ref=block.at[me], dst_ref=block.at[me],
                send_sem=i_send.at[step, at], recv_sem=i_recv.at[step, at],
                device_id={"view": to}, device_id_type=MESH,
            )
            for at, block in enumerate((rbuf, cbuf, wbuf))
        ]

    def build(slot, v, d, i):
        col = cbuf[v, d, pl.ds(i, 1), :].astype(F32)
        fx = (wbuf[v, 1, d, pl.ds(i, 1), :].astype(F32) / 256.0).astype(BF16)
        fx = jnp.broadcast_to(fx, (CHUNK, width))
        for t in range(width // TILE):
            c = jnp.broadcast_to((col - float(t * TILE)).astype(BF16), (CHUNK, width))
            for j in range(TILE // CHUNK):
                apart = (lane_q[pl.ds(j * CHUNK, CHUNK), :] - c) - fx
                mats[slot, pl.ds(t * TILE + j * CHUNK, CHUNK), :] = jnp.maximum(
                    BF16(1.0) - jnp.abs(apart), BF16(0.0)
                )

    def slot_of(v, d, i):
        at = d * rl + i
        return v * (planes * rl) + at if keep else at

    def row_weight(v, d, i):
        row = rbuf[v, d, pl.ds(i, 1), :].astype(F32)
        fy = wbuf[v, 0, d, pl.ds(i, 1), :].astype(F32) / 256.0
        return jnp.maximum(1.0 - jnp.abs(row_of - (row + fy)), 0.0)

    def build_all(v):
        for d in range(planes):
            for i in range(rl):
                build(slot_of(v, d, i), v, d, i)

    def sampled(v, first):
        for s in range(rows):
            for i in range(rl):
                stack[pl.ds((s * rl + i) * cc, cc), :] = fbuf[v, s, :, i, :]
        both_parts = split(stack[...])
        for d in range(planes):
            for i in range(rl):
                if not first:
                    build(slot_of(v, d, i), v, d, i)
                both = jnp.dot(both_parts, mats[slot_of(v, d, i)], preferred_element_type=F32)
                mixed = (both[: height * cc] + both[height * cc :]) * row_weight(v, d, i)
                warped = mixed[:cc]
                for h in range(1, height):
                    warped = warped + mixed[h * cc : (h + 1) * cc]
                warp[v, d, i] = warped
                wsum[d, i] = warped if first else wsum[d, i] + warped

    for copy in local[2:5]:
        copy.wait()
    build_all(me)
    for copy in local[:2]:
        copy.wait()
    pl.semaphore_wait(barrier, views * depths + rows - 2)

    for dr in range(1, rows):
        pass_copy(0, dr).start()

    @pl.loop(1, views)
    def _(step):
        feat_copy(step).start()

    @pl.loop(1, views)
    def _(step):
        for copy in index_copies(step):
            copy.start()

    local[5].wait()
    for d in range(planes):
        for i in range(rl):
            cotg[d, i] = factor * cotv[d, :, i, :]
    for dr in range(1, rows):
        pass_copy(0, dr).wait_recv()
    sampled(me, True)

    @pl.loop(1, views)
    def _(step):
        feat_copy(step).wait_recv()
        for dr in range(1, rows):
            pass_copy(step, dr).start()

    @pl.loop(1, views)
    def _(step):
        for copy in index_copies(step):
            copy.wait_recv()
        for dr in range(1, rows):
            pass_copy(step, dr).wait_recv()
        sampled(view_at(step), False)

    def backward(v):
        if not keep:
            build_all(v)
        both = None
        for d in range(planes):
            for i in range(rl):
                grad = cotg[d, i] * (warp[v, d, i] - wsum[d, i] / views)
                moved = jnp.concatenate([grad] * height, axis=0) * row_weight(v, d, i)
                term = lax.dot_general(
                    split(moved), mats[slot_of(v, d, i)], (((1,), (1,)), ((), ())),
                    preferred_element_type=F32,
                )
                both = term if both is None else both + term
        total = both[: height * cc] + both[height * cc :]
        for s in range(rows):
            for x in range(depths):
                for i in range(rl):
                    at = (s * rl + i) * cc
                    outbuf[v, s, x, i] = total[at : at + cc, x * wx : (x + 1) * wx]

    def core_copy(v, dr):
        r = row_at(dr)
        return pltpu.make_async_remote_copy(
            src_ref=outbuf.at[v, r], dst_ref=pbuf.at[v, dr],
            send_sem=d_send.at[v, dr], recv_sem=d_recv.at[v, dr],
            device_id={"row": r}, device_id_type=MESH,
        )

    def out_copy(v, step, dx):
        x = depth_at(dx)
        return pltpu.make_async_remote_copy(
            src_ref=red.at[v, x], dst_ref=inbuf.at[me, mx],
            send_sem=o_send.at[step, dx], recv_sem=o_recv.at[step, dx],
            device_id={"view": v, "depth": x}, device_id_type=MESH,
        )

    def start_core(v):
        for dr in range(1, rows):
            core_copy(v, dr).start()

    def add_cores(v, target, x):
        piece = outbuf[v, mr, x]
        for dr in range(1, rows):
            piece = piece + pbuf[v, dr, x]
        target[...] = piece

    def pass_on(step):
        v = view_at(step)
        for dr in range(1, rows):
            core_copy(v, dr).wait_recv()
        for x in range(depths):
            add_cores(v, red.at[v, x], x)
        for dx in range(depths):
            out_copy(v, step, dx).start()

    @pl.loop(1, views)
    def _(step):
        v = view_at(step)
        backward(v)
        start_core(v)

        @pl.when(step > 1)
        def _():
            pass_on(step - 1)

    backward(me)
    start_core(me)
    if views > 1:
        pass_on(views - 1)
    for dr in range(1, rows):
        core_copy(me, dr).wait_recv()
    for dx in range(1, depths):
        add_cores(me, red.at[me, depth_at(dx)], depth_at(dx))
        out_copy(me, 0, dx).start()
    add_cores(me, inbuf.at[me, mx], mx)

    @pl.loop(1, views)
    def _(step):
        for dx in range(depths):
            out_copy(view_at(step), step, dx).wait_recv()

    for dx in range(1, depths):
        out_copy(me, 0, dx).wait_recv()

    for i in range(rl):
        for u in range(views):
            piece = inbuf[u, 0, i]
            for x in range(1, depths):
                piece = piece + inbuf[u, x, i]
            out[i, pl.ds(u * cc, cc), :] = piece

    for dr in range(1, rows):
        pass_copy(0, dr).wait_send()
        core_copy(me, dr).wait_send()
    for dx in range(1, depths):
        out_copy(me, 0, dx).wait_send()

    @pl.loop(1, views)
    def _(step):
        feat_copy(step).wait_send()
        for copy in index_copies(step):
            copy.wait_send()
        for dr in range(1, rows):
            pass_copy(step, dr).wait_send()
            core_copy(view_at(step), dr).wait_send()
        for dx in range(depths):
            out_copy(view_at(step), step, dx).wait_send()


def per_device(features, cotangent, src_row, src_col, fractions):
    views, depths, rows = (lax.axis_size(axis) for axis in ("view", "depth", "row"))
    channels, rl, width = features.shape[1:]
    planes, cc = cotangent.shape[:2]
    height, wx = rows * rl, width // depths
    matrices = views * planes * rl
    keep = matrices * width * width * 2 <= KEEP_BYTES
    sizes = (views, depths, rows, cc, planes, rl, width, keep)
    grad = pl.pallas_call(
        functools.partial(kernel, sizes),
        out_shape=jax.ShapeDtypeStruct((rl, channels, wx), F32),
        in_specs=[pl.BlockSpec(memory_space=pl.ANY)] * 5,
        out_specs=pl.BlockSpec(memory_space=pltpu.VMEM),
        scratch_shapes=[
            pltpu.VMEM((channels, rl, width), F32),
            pltpu.VMEM((views, rows, cc, rl, width), F32),
            pltpu.VMEM((views, planes, rl, width), jnp.int32),
            pltpu.VMEM((views, planes, rl, width), jnp.int32),
            pltpu.VMEM((views, 2, planes, rl, width), jnp.int32),
            pltpu.VMEM((planes, cc, rl, width), F32),
            pltpu.VMEM((TILE, width), BF16),
            pltpu.VMEM((height * cc, width), F32),
            pltpu.VMEM((matrices if keep else planes * rl, width, width), BF16),
            pltpu.VMEM((views, planes, rl, cc, width), F32),
            pltpu.VMEM((planes, rl, cc, width), F32),
            pltpu.VMEM((planes, rl, cc, width), F32),
            pltpu.VMEM((views, rows, depths, rl, cc, wx), F32),
            pltpu.VMEM((views, rows, depths, rl, cc, wx), F32),
            pltpu.VMEM((views, depths, rl, cc, wx), F32),
            pltpu.VMEM((views, depths, rl, cc, wx), F32),
            pltpu.SemaphoreType.DMA((6,)),
            pltpu.SemaphoreType.DMA((views,)),
            pltpu.SemaphoreType.DMA((views,)),
            pltpu.SemaphoreType.DMA((views, rows)),
            pltpu.SemaphoreType.DMA((views, rows)),
            pltpu.SemaphoreType.DMA((views, 3)),
            pltpu.SemaphoreType.DMA((views, 3)),
            pltpu.SemaphoreType.DMA((views, rows)),
            pltpu.SemaphoreType.DMA((views, rows)),
            pltpu.SemaphoreType.DMA((views, depths)),
            pltpu.SemaphoreType.DMA((views, depths)),
        ],
        compiler_params=pltpu.CompilerParams(
            collective_id=0, has_side_effects=True, vmem_limit_bytes=56 << 20
        ),
    )(features, cotangent, src_row, src_col, fractions)
    return jnp.transpose(grad, (1, 0, 2))[None]


def solution(mesh):
    in_specs = (
        P("view", None, ("group", "row"), None),
        P("depth", "view", ("group", "row"), None),
        P("view", "depth", ("group", "row"), None),
        P("view", "depth", ("group", "row"), None),
        P(None, "view", "depth", ("group", "row"), None),
    )
    out_specs = P("view", None, ("group", "row"), "depth")
    return jax.shard_map(
        per_device, mesh=mesh, in_specs=in_specs, out_specs=out_specs, check_vma=False
    )
```

```python
import functools

import jax
import jax.numpy as jnp
from jax import lax
from jax.experimental import pallas as pl
from jax.experimental.pallas import tpu as pltpu
from jax.sharding import PartitionSpec as P

MESH = pl.DeviceIdType.MESH
F32 = jnp.float32
BF16 = jnp.bfloat16
TILE = 256
CHUNK = 64
KEEP_BYTES = 24 << 20


def split(value):
    high = value.astype(BF16)
    low = (value - high.astype(F32)).astype(BF16)
    return jnp.concatenate([high, low], axis=0)


def kernel(
    sizes, feat, cot, srow, scol, frac, out,
    fown, fbuf, rbuf, cbuf, wbuf, cotv, lane_q, stack, mats, warp, wsum, cotg, fstack, partial, outbuf, pbuf, red, inbuf,
    local_sem, f_send, f_recv, p_send, p_recv, i_send, i_recv, d_send, d_recv, o_send, o_recv,
):
    views, depths, rows, cc, planes, rl, width, keep, groups = sizes
    me = lax.axis_index("view")
    mx = lax.axis_index("depth")
    mr = lax.axis_index("row")
    height = rows * rl
    wx = width // depths
    factor = 2.0 / views

    def view_at(step):
        return lax.rem(me + step, views)

    def row_at(step):
        return lax.rem(mr + step, rows)

    def depth_at(step):
        return lax.rem(mx + step, depths)

    barrier = pltpu.get_barrier_semaphore()

    def greet(v, x, r):
        pl.semaphore_signal(
            barrier, inc=1, device_id={"view": v, "depth": x, "row": r}, device_id_type=MESH
        )

    @pl.loop(1, views)
    def _(step):
        for dx in range(depths):
            greet(view_at(step), depth_at(dx), mr)

    for dx in range(1, depths):
        greet(me, depth_at(dx), mr)
    for dr in range(1, rows):
        greet(me, mx, row_at(dr))

    local = [
        pltpu.make_async_copy(feat.at[0], fown, local_sem.at[0]),
        pltpu.make_async_copy(feat.at[0, pl.ds(me * cc, cc)], fbuf.at[me, mr], local_sem.at[1]),
        pltpu.make_async_copy(srow.at[0], rbuf.at[me], local_sem.at[2]),
        pltpu.make_async_copy(scol.at[0], cbuf.at[me], local_sem.at[3]),
        pltpu.make_async_copy(frac.at[:, 0], wbuf.at[me], local_sem.at[4]),
        pltpu.make_async_copy(cot, cotv, local_sem.at[5]),
    ]
    for copy in local:
        copy.start()
    for j in range(TILE // CHUNK):
        part = lax.broadcasted_iota(jnp.int32, (CHUNK, width), 0) + j * CHUNK
        lane_q[pl.ds(j * CHUNK, CHUNK), :] = part.astype(F32).astype(BF16)
    row_of = (lax.broadcasted_iota(jnp.int32, (height * cc, width), 0) // cc).astype(F32)

    def feat_copy(step):
        to = lax.rem(me + views - step, views)
        return pltpu.make_async_remote_copy(
            src_ref=fown.at[pl.ds(to * cc, cc)], dst_ref=fbuf.at[me, mr],
            send_sem=f_send.at[step], recv_sem=f_recv.at[step],
            device_id={"view": to}, device_id_type=MESH,
        )

    def pass_copy(step, dr):
        block = fbuf.at[view_at(step), mr]
        return pltpu.make_async_remote_copy(
            src_ref=block, dst_ref=block,
            send_sem=p_send.at[step, dr], recv_sem=p_recv.at[step, dr],
            device_id={"row": row_at(dr)}, device_id_type=MESH,
        )

    per_group = planes // groups

    def index_copies(step, group):
        to = lax.rem(me + views - step, views)
        part = pl.ds(group * per_group, per_group)
        blocks = (rbuf.at[me, part], cbuf.at[me, part], wbuf.at[me, 0, part], wbuf.at[me, 1, part])
        return [
            pltpu.make_async_remote_copy(
                src_ref=block, dst_ref=block,
                send_sem=i_send.at[step, group, at], recv_sem=i_recv.at[step, group, at],
                device_id={"view": to}, device_id_type=MESH,
            )
            for at, block in enumerate(blocks)
        ]

    def build(slot, v, d, i):
        col = cbuf[v, d, pl.ds(i, 1), :].astype(F32)
        fx = (wbuf[v, 1, d, pl.ds(i, 1), :].astype(F32) / 256.0).astype(BF16)
        fx = jnp.broadcast_to(fx, (CHUNK, width))
        for t in range(width // TILE):
            c = jnp.broadcast_to((col - float(t * TILE)).astype(BF16), (CHUNK, width))
            for j in range(TILE // CHUNK):
                apart = (lane_q[pl.ds(j * CHUNK, CHUNK), :] - c) - fx
                mats[slot, pl.ds(t * TILE + j * CHUNK, CHUNK), :] = jnp.maximum(
                    BF16(1.0) - jnp.abs(apart), BF16(0.0)
                )

    def slot_of(v, d, i):
        at = d * rl + i
        return v * (planes * rl) + at if keep else at

    def row_weight(v, d, i):
        row = rbuf[v, d, pl.ds(i, 1), :].astype(F32)
        fy = wbuf[v, 0, d, pl.ds(i, 1), :].astype(F32) / 256.0
        return jnp.maximum(1.0 - jnp.abs(row_of - (row + fy)), 0.0)

    def planes_of(group):
        return range(group * per_group, (group + 1) * per_group)

    def build_all(v, plane_list):
        for d in plane_list:
            for i in range(rl):
                build(slot_of(v, d, i), v, d, i)

    def load_features(v):
        for s in range(rows):
            for i in range(rl):
                stack[pl.ds((s * rl + i) * cc, cc), :] = fbuf[v, s, :, i, :]
        fstack[v] = split(stack[...])

    def sampled(v, plane_list, first):
        for d in plane_list:
            for i in range(rl):
                if not first:
                    build(slot_of(v, d, i), v, d, i)
                both = jnp.dot(fstack[v], mats[slot_of(v, d, i)], preferred_element_type=F32)
                mixed = (both[: height * cc] + both[height * cc :]) * row_weight(v, d, i)
                warped = mixed[:cc]
                for h in range(1, height):
                    warped = warped + mixed[h * cc : (h + 1) * cc]
                warp[v, d, i] = warped
                wsum[d, i] = warped if first else wsum[d, i] + warped

    for copy in local[2:5]:
        copy.wait()
    build_all(me, range(planes))
    for copy in local[:2]:
        copy.wait()
    pl.semaphore_wait(barrier, views * depths + rows - 2)

    for dr in range(1, rows):
        pass_copy(0, dr).start()

    @pl.loop(1, views)
    def _(step):
        feat_copy(step).start()

    for group in range(groups):

        @pl.loop(1, views)
        def _(step):
            for copy in index_copies(step, group):
                copy.start()

    local[5].wait()
    for d in range(planes):
        for i in range(rl):
            cotg[d, i] = factor * cotv[d, :, i, :]
    for dr in range(1, rows):
        pass_copy(0, dr).wait_recv()
    load_features(me)
    sampled(me, range(planes), True)

    @pl.loop(1, views)
    def _(step):
        feat_copy(step).wait_recv()
        for dr in range(1, rows):
            pass_copy(step, dr).start()

    def gather_group(group):
        @pl.loop(1, views)
        def _(step):
            for copy in index_copies(step, group):
                copy.wait_recv()
            if group == 0:
                for dr in range(1, rows):
                    pass_copy(step, dr).wait_recv()
                load_features(view_at(step))
            sampled(view_at(step), planes_of(group), False)

    def adjoint(v, plane_list):
        if not keep:
            build_all(v, plane_list)
        both = None
        for d in plane_list:
            for i in range(rl):
                grad = cotg[d, i] * (warp[v, d, i] - wsum[d, i] / views)
                moved = jnp.concatenate([grad] * height, axis=0) * row_weight(v, d, i)
                term = lax.dot_general(
                    split(moved), mats[slot_of(v, d, i)], (((1,), (1,)), ((), ())),
                    preferred_element_type=F32,
                )
                both = term if both is None else both + term
        return both[: height * cc] + both[height * cc :]

    for group in range(groups - 1):
        gather_group(group)

        @pl.loop(0, views)
        def _(v):
            term = adjoint(v, planes_of(group))
            partial[v] = term if group == 0 else partial[v] + term

    gather_group(groups - 1)

    def backward(v):
        total = adjoint(v, planes_of(groups - 1))
        if groups > 1:
            total = total + partial[v]
        for s in range(rows):
            for x in range(depths):
                for i in range(rl):
                    at = (s * rl + i) * cc
                    outbuf[v, s, x, i] = total[at : at + cc, x * wx : (x + 1) * wx]

    def core_copy(v, dr):
        r = row_at(dr)
        return pltpu.make_async_remote_copy(
            src_ref=outbuf.at[v, r], dst_ref=pbuf.at[v, dr],
            send_sem=d_send.at[v, dr], recv_sem=d_recv.at[v, dr],
            device_id={"row": r}, device_id_type=MESH,
        )

    def out_copy(v, step, dx):
        x = depth_at(dx)
        return pltpu.make_async_remote_copy(
            src_ref=red.at[v, x], dst_ref=inbuf.at[me, mx],
            send_sem=o_send.at[step, dx], recv_sem=o_recv.at[step, dx],
            device_id={"view": v, "depth": x}, device_id_type=MESH,
        )

    def start_core(v):
        for dr in range(1, rows):
            core_copy(v, dr).start()

    def add_cores(v, target, x):
        piece = outbuf[v, mr, x]
        for dr in range(1, rows):
            piece = piece + pbuf[v, dr, x]
        target[...] = piece

    def pass_on(step):
        v = view_at(step)
        for dr in range(1, rows):
            core_copy(v, dr).wait_recv()
        for x in range(depths):
            add_cores(v, red.at[v, x], x)
        for dx in range(depths):
            out_copy(v, step, dx).start()

    @pl.loop(1, views)
    def _(step):
        v = view_at(step)
        backward(v)
        start_core(v)

        @pl.when(step > 1)
        def _():
            pass_on(step - 1)

    backward(me)
    start_core(me)
    if views > 1:
        pass_on(views - 1)
    for dr in range(1, rows):
        core_copy(me, dr).wait_recv()
    for dx in range(1, depths):
        add_cores(me, red.at[me, depth_at(dx)], depth_at(dx))
        out_copy(me, 0, dx).start()
    add_cores(me, inbuf.at[me, mx], mx)

    @pl.loop(1, views)
    def _(step):
        for dx in range(depths):
            out_copy(view_at(step), step, dx).wait_recv()

    for dx in range(1, depths):
        out_copy(me, 0, dx).wait_recv()

    for i in range(rl):
        for u in range(views):
            piece = inbuf[u, 0, i]
            for x in range(1, depths):
                piece = piece + inbuf[u, x, i]
            out[i, pl.ds(u * cc, cc), :] = piece

    for dr in range(1, rows):
        pass_copy(0, dr).wait_send()
        core_copy(me, dr).wait_send()
    for dx in range(1, depths):
        out_copy(me, 0, dx).wait_send()

    @pl.loop(1, views)
    def _(step):
        feat_copy(step).wait_send()
        for group in range(groups):
            for copy in index_copies(step, group):
                copy.wait_send()
        for dr in range(1, rows):
            pass_copy(step, dr).wait_send()
            core_copy(view_at(step), dr).wait_send()
        for dx in range(depths):
            out_copy(view_at(step), step, dx).wait_send()


def per_device(features, cotangent, src_row, src_col, fractions):
    views, depths, rows = (lax.axis_size(axis) for axis in ("view", "depth", "row"))
    channels, rl, width = features.shape[1:]
    planes, cc = cotangent.shape[:2]
    height, wx = rows * rl, width // depths
    matrices = views * planes * rl
    keep = matrices * width * width * 2 <= KEEP_BYTES
    groups = 2 if planes % 2 == 0 else 1
    sizes = (views, depths, rows, cc, planes, rl, width, keep, groups)
    grad = pl.pallas_call(
        functools.partial(kernel, sizes),
        out_shape=jax.ShapeDtypeStruct((rl, channels, wx), F32),
        in_specs=[pl.BlockSpec(memory_space=pl.ANY)] * 5,
        out_specs=pl.BlockSpec(memory_space=pltpu.VMEM),
        scratch_shapes=[
            pltpu.VMEM((channels, rl, width), F32),
            pltpu.VMEM((views, rows, cc, rl, width), F32),
            pltpu.VMEM((views, planes, rl, width), jnp.int32),
            pltpu.VMEM((views, planes, rl, width), jnp.int32),
            pltpu.VMEM((views, 2, planes, rl, width), jnp.int32),
            pltpu.VMEM((planes, cc, rl, width), F32),
            pltpu.VMEM((TILE, width), BF16),
            pltpu.VMEM((height * cc, width), F32),
            pltpu.VMEM((matrices if keep else planes * rl, width, width), BF16),
            pltpu.VMEM((views, planes, rl, cc, width), F32),
            pltpu.VMEM((planes, rl, cc, width), F32),
            pltpu.VMEM((planes, rl, cc, width), F32),
            pltpu.VMEM((views, 2 * height * cc, width), BF16),
            pltpu.VMEM((views, height * cc, width), F32),
            pltpu.VMEM((views, rows, depths, rl, cc, wx), F32),
            pltpu.VMEM((views, rows, depths, rl, cc, wx), F32),
            pltpu.VMEM((views, depths, rl, cc, wx), F32),
            pltpu.VMEM((views, depths, rl, cc, wx), F32),
            pltpu.SemaphoreType.DMA((6,)),
            pltpu.SemaphoreType.DMA((views,)),
            pltpu.SemaphoreType.DMA((views,)),
            pltpu.SemaphoreType.DMA((views, rows)),
            pltpu.SemaphoreType.DMA((views, rows)),
            pltpu.SemaphoreType.DMA((views, groups, 4)),
            pltpu.SemaphoreType.DMA((views, groups, 4)),
            pltpu.SemaphoreType.DMA((views, rows)),
            pltpu.SemaphoreType.DMA((views, rows)),
            pltpu.SemaphoreType.DMA((views, depths)),
            pltpu.SemaphoreType.DMA((views, depths)),
        ],
        compiler_params=pltpu.CompilerParams(
            collective_id=0, has_side_effects=True, vmem_limit_bytes=56 << 20
        ),
    )(features, cotangent, src_row, src_col, fractions)
    return jnp.transpose(grad, (1, 0, 2))[None]


def solution(mesh):
    in_specs = (
        P("view", None, ("group", "row"), None),
        P("depth", "view", ("group", "row"), None),
        P("view", "depth", ("group", "row"), None),
        P("view", "depth", ("group", "row"), None),
        P(None, "view", "depth", ("group", "row"), None),
    )
    out_specs = P("view", None, ("group", "row"), "depth")
    return jax.shard_map(
        per_device, mesh=mesh, in_specs=in_specs, out_specs=out_specs, check_vma=False
    )
```

```python
import functools

import jax
import jax.numpy as jnp
from jax import lax
from jax.experimental import pallas as pl
from jax.experimental.pallas import tpu as pltpu
from jax.sharding import PartitionSpec as P

MESH = pl.DeviceIdType.MESH
F32 = jnp.float32
BF16 = jnp.bfloat16
TILE = 256
CHUNK = 64
KEEP_BYTES = 24 << 20


def split(value):
    high = value.astype(BF16)
    low = (value - high.astype(F32)).astype(BF16)
    return jnp.concatenate([high, low], axis=0)


def kernel(
    sizes, feat, cot, srow, scol, frac, out,
    fown, fbuf, rbuf, cbuf, wbuf, cotv, lane_q, stack, mats, warp, wsum, cotg, outbuf, pbuf, red, inbuf,
    local_sem, f_send, f_recv, p_send, p_recv, i_send, i_recv, d_send, d_recv, o_send, o_recv,
):
    views, depths, rows, cc, planes, rl, width, keep = sizes
    me = lax.axis_index("view")
    mx = lax.axis_index("depth")
    mr = lax.axis_index("row")
    height = rows * rl
    wx = width // depths
    factor = 2.0 / views

    def view_at(step):
        return lax.rem(me + step, views)

    def row_at(step):
        return lax.rem(mr + step, rows)

    def depth_at(step):
        return lax.rem(mx + step, depths)

    barrier = pltpu.get_barrier_semaphore()

    def greet(v, x, r):
        pl.semaphore_signal(
            barrier, inc=1, device_id={"view": v, "depth": x, "row": r}, device_id_type=MESH
        )

    @pl.loop(1, views)
    def _(step):
        greet(view_at(step), mx, mr)

    for dx in range(1, depths):
        greet(me, depth_at(dx), mr)
    for dr in range(1, rows):
        greet(me, mx, row_at(dr))

    local = [
        pltpu.make_async_copy(feat.at[0], fown, local_sem.at[0]),
        pltpu.make_async_copy(feat.at[0, pl.ds(me * cc, cc)], fbuf.at[me, mr], local_sem.at[1]),
        pltpu.make_async_copy(srow.at[0], rbuf.at[me], local_sem.at[2]),
        pltpu.make_async_copy(scol.at[0], cbuf.at[me], local_sem.at[3]),
        pltpu.make_async_copy(frac.at[:, 0], wbuf.at[me], local_sem.at[4]),
        pltpu.make_async_copy(cot, cotv, local_sem.at[5]),
    ]
    for copy in local:
        copy.start()
    for j in range(TILE // CHUNK):
        part = lax.broadcasted_iota(jnp.int32, (CHUNK, width), 0) + j * CHUNK
        lane_q[pl.ds(j * CHUNK, CHUNK), :] = part.astype(F32).astype(BF16)
    row_of = (lax.broadcasted_iota(jnp.int32, (height * cc, width), 0) // cc).astype(F32)

    def feat_copy(step):
        to = lax.rem(me + views - step, views)
        return pltpu.make_async_remote_copy(
            src_ref=fown.at[pl.ds(to * cc, cc)], dst_ref=fbuf.at[me, mr],
            send_sem=f_send.at[step], recv_sem=f_recv.at[step],
            device_id={"view": to}, device_id_type=MESH,
        )

    def pass_copy(step, dr):
        block = fbuf.at[view_at(step), mr]
        return pltpu.make_async_remote_copy(
            src_ref=block, dst_ref=block,
            send_sem=p_send.at[step, dr], recv_sem=p_recv.at[step, dr],
            device_id={"row": row_at(dr)}, device_id_type=MESH,
        )

    def index_copies(step):
        to = lax.rem(me + views - step, views)
        return [
            pltpu.make_async_remote_copy(
                src_ref=block.at[me], dst_ref=block.at[me],
                send_sem=i_send.at[step, at], recv_sem=i_recv.at[step, at],
                device_id={"view": to}, device_id_type=MESH,
            )
            for at, block in enumerate((rbuf, cbuf, wbuf))
        ]

    def build(slot, v, d, i):
        col = cbuf[v, d, pl.ds(i, 1), :].astype(F32)
        fx = (wbuf[v, 1, d, pl.ds(i, 1), :].astype(F32) / 256.0).astype(BF16)
        fx = jnp.broadcast_to(fx, (CHUNK, width))
        for t in range(width // TILE):
            c = jnp.broadcast_to((col - float(t * TILE)).astype(BF16), (CHUNK, width))
            for j in range(TILE // CHUNK):
                apart = (lane_q[pl.ds(j * CHUNK, CHUNK), :] - c) - fx
                mats[slot, pl.ds(t * TILE + j * CHUNK, CHUNK), :] = jnp.maximum(
                    BF16(1.0) - jnp.abs(apart), BF16(0.0)
                )

    def slot_of(v, d, i):
        at = d * rl + i
        return v * (planes * rl) + at if keep else at

    def row_weight(v, d, i):
        row = rbuf[v, d, pl.ds(i, 1), :].astype(F32)
        fy = wbuf[v, 0, d, pl.ds(i, 1), :].astype(F32) / 256.0
        return jnp.maximum(1.0 - jnp.abs(row_of - (row + fy)), 0.0)

    def build_all(v):
        for d in range(planes):
            for i in range(rl):
                build(slot_of(v, d, i), v, d, i)

    def sampled(v, first):
        for s in range(rows):
            for i in range(rl):
                stack[pl.ds((s * rl + i) * cc, cc), :] = fbuf[v, s, :, i, :]
        both_parts = split(stack[...])
        for d in range(planes):
            for i in range(rl):
                if not first:
                    build(slot_of(v, d, i), v, d, i)
                both = jnp.dot(both_parts, mats[slot_of(v, d, i)], preferred_element_type=F32)
                mixed = (both[: height * cc] + both[height * cc :]) * row_weight(v, d, i)
                warped = mixed[:cc]
                for h in range(1, height):
                    warped = warped + mixed[h * cc : (h + 1) * cc]
                warp[v, d, i] = warped
                wsum[d, i] = warped if first else wsum[d, i] + warped

    for copy in local[2:5]:
        copy.wait()
    build_all(me)
    for copy in local[:2]:
        copy.wait()
    pl.semaphore_wait(barrier, views + depths + rows - 3)

    for dr in range(1, rows):
        pass_copy(0, dr).start()

    @pl.loop(1, views)
    def _(step):
        feat_copy(step).start()

    @pl.loop(1, views)
    def _(step):
        for copy in index_copies(step):
            copy.start()

    local[5].wait()
    for d in range(planes):
        for i in range(rl):
            cotg[d, i] = factor * cotv[d, :, i, :]
    for dr in range(1, rows):
        pass_copy(0, dr).wait_recv()
    sampled(me, True)

    @pl.loop(1, views)
    def _(step):
        feat_copy(step).wait_recv()
        for dr in range(1, rows):
            pass_copy(step, dr).start()

    @pl.loop(1, views)
    def _(step):
        for copy in index_copies(step):
            copy.wait_recv()
        for dr in range(1, rows):
            pass_copy(step, dr).wait_recv()
        sampled(view_at(step), False)

    def backward(v):
        if not keep:
            build_all(v)
        both = None
        for d in range(planes):
            for i in range(rl):
                grad = cotg[d, i] * (warp[v, d, i] - wsum[d, i] / views)
                moved = jnp.concatenate([grad] * height, axis=0) * row_weight(v, d, i)
                term = lax.dot_general(
                    split(moved), mats[slot_of(v, d, i)], (((1,), (1,)), ((), ())),
                    preferred_element_type=F32,
                )
                both = term if both is None else both + term
        total = both[: height * cc] + both[height * cc :]
        for s in range(rows):
            for x in range(depths):
                for i in range(rl):
                    at = (s * rl + i) * cc
                    outbuf[v, s, x, i] = total[at : at + cc, x * wx : (x + 1) * wx]

    def core_copy(v, dr):
        r = row_at(dr)
        return pltpu.make_async_remote_copy(
            src_ref=outbuf.at[v, r], dst_ref=pbuf.at[v, dr],
            send_sem=d_send.at[v, dr], recv_sem=d_recv.at[v, dr],
            device_id={"row": r}, device_id_type=MESH,
        )

    def out_copy(v, step, dx):
        x = depth_at(dx)
        return pltpu.make_async_remote_copy(
            src_ref=red.at[v, x], dst_ref=inbuf.at[me, mx],
            send_sem=o_send.at[step, dx], recv_sem=o_recv.at[step, dx],
            device_id={"view": v, "depth": x}, device_id_type=MESH,
        )

    def start_core(v):
        for dr in range(1, rows):
            core_copy(v, dr).start()

    def add_cores(v, target, x):
        piece = outbuf[v, mr, x]
        for dr in range(1, rows):
            piece = piece + pbuf[v, dr, x]
        target[...] = piece

    def pass_on(step):
        v = view_at(step)
        for dr in range(1, rows):
            core_copy(v, dr).wait_recv()
        for x in range(depths):
            add_cores(v, red.at[v, x], x)
        for dx in range(depths):
            out_copy(v, step, dx).start()

    @pl.loop(1, views)
    def _(step):
        v = view_at(step)
        backward(v)
        start_core(v)

        @pl.when(step > 1)
        def _():
            pass_on(step - 1)

    backward(me)
    start_core(me)
    if views > 1:
        pass_on(views - 1)
    for dr in range(1, rows):
        core_copy(me, dr).wait_recv()
    for dx in range(1, depths):
        add_cores(me, red.at[me, depth_at(dx)], depth_at(dx))
        out_copy(me, 0, dx).start()
    add_cores(me, inbuf.at[me, mx], mx)

    @pl.loop(1, views)
    def _(step):
        for dx in range(depths):
            out_copy(view_at(step), step, dx).wait_recv()

    for dx in range(1, depths):
        out_copy(me, 0, dx).wait_recv()

    for i in range(rl):
        for u in range(views):
            piece = inbuf[u, 0, i]
            for x in range(1, depths):
                piece = piece + inbuf[u, x, i]
            out[i, pl.ds(u * cc, cc), :] = piece

    for dr in range(1, rows):
        pass_copy(0, dr).wait_send()
        core_copy(me, dr).wait_send()
    for dx in range(1, depths):
        out_copy(me, 0, dx).wait_send()

    @pl.loop(1, views)
    def _(step):
        feat_copy(step).wait_send()
        for copy in index_copies(step):
            copy.wait_send()
        for dr in range(1, rows):
            pass_copy(step, dr).wait_send()
            core_copy(view_at(step), dr).wait_send()
        for dx in range(depths):
            out_copy(view_at(step), step, dx).wait_send()


def per_device(features, cotangent, src_row, src_col, fractions):
    views, depths, rows = (lax.axis_size(axis) for axis in ("view", "depth", "row"))
    channels, rl, width = features.shape[1:]
    planes, cc = cotangent.shape[:2]
    height, wx = rows * rl, width // depths
    matrices = views * planes * rl
    keep = matrices * width * width * 2 <= KEEP_BYTES
    sizes = (views, depths, rows, cc, planes, rl, width, keep)
    grad = pl.pallas_call(
        functools.partial(kernel, sizes),
        out_shape=jax.ShapeDtypeStruct((rl, channels, wx), F32),
        in_specs=[pl.BlockSpec(memory_space=pl.ANY)] * 5,
        out_specs=pl.BlockSpec(memory_space=pltpu.VMEM),
        scratch_shapes=[
            pltpu.VMEM((channels, rl, width), F32),
            pltpu.VMEM((views, rows, cc, rl, width), F32),
            pltpu.VMEM((views, planes, rl, width), jnp.int32),
            pltpu.VMEM((views, planes, rl, width), jnp.int32),
            pltpu.VMEM((views, 2, planes, rl, width), jnp.int32),
            pltpu.VMEM((planes, cc, rl, width), F32),
            pltpu.VMEM((TILE, width), BF16),
            pltpu.VMEM((height * cc, width), F32),
            pltpu.VMEM((matrices if keep else planes * rl, width, width), BF16),
            pltpu.VMEM((views, planes, rl, cc, width), F32),
            pltpu.VMEM((planes, rl, cc, width), F32),
            pltpu.VMEM((planes, rl, cc, width), F32),
            pltpu.VMEM((views, rows, depths, rl, cc, wx), F32),
            pltpu.VMEM((views, rows, depths, rl, cc, wx), F32),
            pltpu.VMEM((views, depths, rl, cc, wx), F32),
            pltpu.VMEM((views, depths, rl, cc, wx), F32),
            pltpu.SemaphoreType.DMA((6,)),
            pltpu.SemaphoreType.DMA((views,)),
            pltpu.SemaphoreType.DMA((views,)),
            pltpu.SemaphoreType.DMA((views, rows)),
            pltpu.SemaphoreType.DMA((views, rows)),
            pltpu.SemaphoreType.DMA((views, 3)),
            pltpu.SemaphoreType.DMA((views, 3)),
            pltpu.SemaphoreType.DMA((views, rows)),
            pltpu.SemaphoreType.DMA((views, rows)),
            pltpu.SemaphoreType.DMA((views, depths)),
            pltpu.SemaphoreType.DMA((views, depths)),
        ],
        compiler_params=pltpu.CompilerParams(
            collective_id=0, has_side_effects=True, vmem_limit_bytes=56 << 20
        ),
    )(features, cotangent, src_row, src_col, fractions)
    return jnp.transpose(grad, (1, 0, 2))[None]


def solution(mesh):
    in_specs = (
        P("view", None, ("group", "row"), None),
        P("depth", "view", ("group", "row"), None),
        P("view", "depth", ("group", "row"), None),
        P("view", "depth", ("group", "row"), None),
        P(None, "view", "depth", ("group", "row"), None),
    )
    out_specs = P("view", None, ("group", "row"), "depth")
    return jax.shard_map(
        per_device, mesh=mesh, in_specs=in_specs, out_specs=out_specs, check_vma=False
    )
```
